128 devices in a mesh: items: 32 (over y, z, core), users: 4 (over x).
Axes of the slice: x: 4, y: 4, z: 4, core: 2. Of those that a mesh axis runs over, the one named last changes fastest.
Arguments:
- user_emb: bfloat16 [4096, 256], P('users', 'items'), as said below
- item_emb: bfloat16 [1048576, 256], P('items'), as said below
- target: int32 [4096], P('users'), may hold values from 0 to 1048575
- history: int32 [4096, 32], P('users'), may hold values from 0 to 1048575, as said below
Outputs:
- log_rank: float32 [4096], P('users')
- metrics: float32 [2], replicated
The draws below stay inside these ranges and needn't reach their ends.
Inputs may be any that keep to these rules, and one draw needn't show every extreme that they name: history[u, k] lies in [k * 32768, (k + 1) * 32768); a user's history entries are thus distinct. `item_emb`: rows of norm about one. `user_emb`: entries of order one.
All inputs are finite; a program needn't handle non-finite values.
Results may differ from the reference program's by a relative error of at most 0.0003.
Values may be sent and summed in bfloat16 or wider, within the bound.
A program may use at most 64 MiB of HBM per device.

```python
import jax
import jax.numpy as jnp
from jax import lax

D = 256
H = 32
ITEMS = 1048576
USERS = 4096


def item_row(base, row):
    return jax.random.normal(jax.random.fold_in(base, row), (D,), jnp.float32) / jnp.sqrt(float(D))


def shared_ints(key):
    target = jax.random.randint(jax.random.fold_in(key, 12), (USERS,), 0, ITEMS).astype(jnp.int32)
    stride = ITEMS // H
    offset = jax.random.randint(jax.random.fold_in(key, 13), (USERS, H), 0, stride).astype(jnp.int32)
    history = offset + (jnp.arange(H, dtype=jnp.int32) * stride)[None, :]
    return (target, history)


def draw_item_emb(key, part):
    base = jax.random.fold_in(key, 11)
    rows = jax.vmap(lambda r: item_row(base, r))(jnp.arange(ITEMS, dtype=jnp.int32))
    return rows.astype(jnp.bfloat16)


def draw_target(key, part):
    return shared_ints(key)[0]


def draw_history(key, part):
    return shared_ints(key)[1]


def draw_user_emb(key, part):
    base = jax.random.fold_in(key, 11)
    target, history = shared_ints(key)
    trow = jax.vmap(lambda r: item_row(base, r))(target)
    hrows = jax.vmap(jax.vmap(lambda r: item_row(base, r)))(history)
    noise = jax.random.normal(jax.random.fold_in(key, 14), (USERS, D), jnp.float32) * 0.6
    query = noise + 4.0 * trow + 2.5 * jnp.sum(hrows, axis=1)
    return query.astype(jnp.bfloat16)


def setup_inputs(seed: int = 0) -> dict:
    key_of = jax.random.split(jax.random.key(seed), 5)
    return {
        "user_emb": draw_user_emb(jax.random.fold_in(key_of[4], 71), 0),
        "item_emb": draw_item_emb(jax.random.fold_in(key_of[4], 71), 0),
        "target": draw_target(jax.random.fold_in(key_of[4], 71), 0),
        "history": draw_history(jax.random.fold_in(key_of[4], 71), 0),
    }


sharpness = 4.0


def reference(user_emb, item_emb, target, history):
    users = user_emb.astype(jnp.float32)
    items = item_emb.astype(jnp.float32)
    tscore = jnp.sum(users * items[target], axis=1)
    blk = min(ITEMS, 8192)
    nblk = ITEMS // blk
    blocks = items.reshape(nblk, blk, D)

    def step(total, rows):
        score = jnp.dot(users, rows.T, preferred_element_type=jnp.float32, precision=lax.Precision.HIGHEST)
        return total + jnp.sum(jax.nn.sigmoid(sharpness * (score - tscore[:, None])), axis=1), None

    total, _ = lax.scan(step, jnp.zeros((USERS,), jnp.float32), blocks)
    hrows = items[history]
    hscore = jnp.einsum("ud,uhd->uh", users, hrows, precision=lax.Precision.HIGHEST)
    seen_sum = jnp.sum(jax.nn.sigmoid(sharpness * (hscore - tscore[:, None])), axis=1)
    seen = jnp.any(history == target[:, None], axis=1)
    above = total - seen_sum - jnp.where(seen, 0.0, 0.5).astype(jnp.float32)
    rank = 1.0 + above
    log_rank = jnp.log(rank)
    hit = jax.nn.sigmoid(10.5 - rank)
    gain = hit / jnp.log2(1.0 + rank)
    metrics = jnp.stack([jnp.sum(hit), jnp.sum(gain)]) / USERS
    return log_rank, metrics
```

```python
import functools

import jax
import jax.numpy as jnp
from jax import lax
from jax.experimental import pallas as pl
from jax.experimental.pallas import tpu as pltpu
from jax.sharding import PartitionSpec as P

MESH = pl.DeviceIdType.MESH
CHUNK = 4096
PARTS = 2
PIECES = 8
BATCH = 16
TILE = 16


def exchange(axis, n, me, src, dst, send, recv):
    copies = []
    for off in range(1, n):
        peer = lax.rem(me + off, n)
        copies.append(
            pltpu.make_async_remote_copy(
                src_ref=src,
                dst_ref=dst,
                send_sem=send.at[off - 1],
                recv_sem=recv.at[off - 1],
                device_id={axis: peer},
                device_id_type=MESH,
            )
        )
    for c in copies:
        c.start()
    return copies


def collect(ids, row, items, rows):
    tiles = items.shape[0]

    def body(i, carry):
        for j in range(BATCH):
            user = i * BATCH + j
            rows[user] = items[lax.rem(lax.div(ids[row, user], TILE), tiles)]
        return carry

    lax.fori_loop(0, ids.shape[1] // BATCH, body, 0)


def own_scores(rows, w, ids, at, width):
    lane = lax.broadcasted_iota(jnp.int32, (TILE, 128), 1)
    sub = lax.broadcasted_iota(jnp.int32, (TILE, 128), 0)
    d = rows.shape[2]
    out = []
    for b in range(width // 128):
        lo = at + b * 128
        pc = jnp.dot(
            rows[lo : lo + 128].reshape(128 * TILE, d), w[:, lo : lo + 128], preferred_element_type=jnp.float32
        )
        got = pc[:TILE]
        for r in range(1, 128):
            got = jnp.where(lane == r, pc[TILE * r : TILE * (r + 1)], got)
        here = sub == (ids[:, b * 128 : (b + 1) * 128] & (TILE - 1))
        out.append(jnp.sum(jnp.where(here, got, 0.0), axis=0, keepdims=True))
    return jnp.concatenate(out, axis=1)


def kernel(
    n, m, u_hbm, item_ref, tgt_hbm, hist_hbm, log_ref, met_ref,
    u_ref, tgt_ref, hist_ref, tid_ref, hid_ref, gath, w, items, rows, sa, sb, tpart, tslots, apart, aslots, mpart, mslots, hsc,
    sem_item, sem_in, us, ur, ts, tr, as_, ar, ms, mr,
):
    me = lax.axis_index("items")
    grp = lax.axis_index("users")
    dsh, u_dev = u_ref.shape
    d = item_ref.shape[2]
    item_dev = item_ref.shape[0] * TILE
    half = u_dev // PARTS
    piece = item_dev // TILE // PIECES

    ins = [
        pltpu.make_async_copy(u_hbm, u_ref, sem_in.at[0]),
        pltpu.make_async_copy(tgt_hbm, tgt_ref, sem_in.at[1]),
        pltpu.make_async_copy(hist_hbm, hist_ref, sem_in.at[2]),
        pltpu.make_async_copy(tgt_hbm, tid_ref, sem_in.at[3]),
        pltpu.make_async_copy(hist_hbm.at[pl.ds(pl.multiple_of(lax.div(me, 8) * 8, 8), 8), :], hid_ref, sem_in.at[4]),
    ]
    for c in ins:
        c.start()
    fetches = []
    for i in range(PIECES):
        part = pl.ds(i * piece, piece)
        fetches.append(pltpu.make_async_copy(item_ref.at[part], items.at[part], sem_item.at[i]))
    for f in fetches:
        f.start()

    barrier = pltpu.get_barrier_semaphore()
    for off in range(1, n):
        pl.semaphore_signal(barrier, inc=1, device_id={"items": lax.rem(me + off, n)}, device_id_type=MESH)
    for off in range(1, m):
        pl.semaphore_signal(barrier, inc=1, device_id={"users": lax.rem(grp + off, m)}, device_id_type=MESH)
    pl.semaphore_wait(barrier, n - 1 + m - 1)

    for c in ins:
        c.wait()
    ucopies = []
    for p in range(PARTS):
        cols = slice(p * half, (p + 1) * half)
        ucopies.append(exchange("items", n, me, u_ref.at[:, cols], gath.at[p, me], us.at[p], ur.at[p]))
        gath[p, me] = u_ref[:, cols]

    for f in fetches:
        f.wait()
    collect(tid_ref, 0, items, rows)

    tcopies = []
    for p in range(PARTS):
        for c in ucopies[p]:
            c.wait()
        cols = slice(p * half, (p + 1) * half)
        for i in range(n):
            w[i * dsh : (i + 1) * dsh, cols] = gath[p, i] * jnp.bfloat16(2)
        tgt = tgt_ref[:, cols]
        got = own_scores(rows, w, tgt, p * half, half)
        local = tgt - me * item_dev
        tpart[p] = jnp.where((local >= 0) & (local < item_dev), got, 0.0)
        tslots[p, me] = tpart[p]
        tcopies.append(exchange("items", n, me, tpart.at[p], tslots.at[p, me], ts.at[p], tr.at[p]))

    collect(hid_ref, lax.rem(me, 8), items, rows)
    for p in range(PARTS):
        cols = slice(p * half, (p + 1) * half)
        hsc[:, cols] = own_scores(rows, w, hist_ref[pl.ds(me, 1), cols], p * half, half)

    steps = item_dev // CHUNK

    def score(k, dst):
        at = lax.rem(k, steps) * (CHUNK // TILE)
        col = pl.multiple_of(lax.div(k, steps) * half, half)
        dst[...] = jnp.dot(
            items[pl.ds(at, CHUNK // TILE)].reshape(CHUNK, d), w[:, pl.ds(col, half)], preferred_element_type=jnp.float32
        )

    score(0, sa)
    acopies = []
    for p in range(PARTS):
        cols = slice(p * half, (p + 1) * half)
        for c in tcopies[p]:
            c.wait()
        tsum = tslots[p, 0]
        for i in range(1, n):
            tsum = tsum + tslots[p, i]
        t = jnp.broadcast_to(tsum, (8, half))

        def count(src, acc, t=t):
            sums = []
            for g in range(CHUNK // 8):
                v = jnp.tanh(src[8 * g : 8 * g + 8, :] - t) + 1.0
                lvl = 0
                while sums and sums[-1][0] == lvl and lvl < 3:
                    v = sums.pop()[1] + v
                    lvl += 1
                if lvl == 3:
                    acc = acc + v
                else:
                    sums.append((lvl, v))
            return acc

        def step(i, acc, p=p):
            k = p * steps + 2 * i
            score(k + 1, sb)
            acc = count(sa, acc)
            score(lax.rem(k + 2, PARTS * steps), sa)
            return count(sb, acc)

        acc = lax.fori_loop(0, steps // 2, step, jnp.zeros((8, half), jnp.float32))
        mine = jnp.tanh(hsc[:, cols] - tsum) + 1.0
        apart[p] = 0.5 * (jnp.sum(acc, axis=0, keepdims=True) - mine)
        aslots[p, me] = apart[p]
        acopies.append(exchange("items", n, me, apart.at[p], aslots.at[p, me], as_.at[p], ar.at[p]))

    seen = jnp.max(jnp.where(hist_ref[...] == tgt_ref[...], 1.0, 0.0), axis=0, keepdims=True)
    hs = jnp.zeros((1, 128), jnp.float32)
    gs = jnp.zeros((1, 128), jnp.float32)
    for p in range(PARTS):
        cols = slice(p * half, (p + 1) * half)
        for c in acopies[p]:
            c.wait()
        total = aslots[p, 0]
        for i in range(1, n):
            total = total + aslots[p, i]
        rank = 1.0 + (total - jnp.where(seen[:, cols] > 0.5, 0.0, 0.5))
        log_ref[:, cols] = jnp.log(rank)
        hit = jax.nn.sigmoid(10.5 - rank)
        gain = hit / jnp.log2(1.0 + rank)
        for b in range(half // 128):
            hs = hs + hit[:, b * 128 : (b + 1) * 128]
            gs = gs + gain[:, b * 128 : (b + 1) * 128]
    mpart[:, :128] = hs
    mpart[:, 128:] = gs
    mslots[grp] = mpart[...]
    copies = exchange("users", m, grp, mpart, mslots.at[grp], ms, mr)
    for c in copies:
        c.wait()
    tot = mslots[0]
    for i in range(1, m):
        tot = tot + mslots[i]
    scale = 1.0 / (u_dev * m)
    met_ref[0] = jnp.sum(tot[:, :128]) * scale
    met_ref[1] = jnp.sum(tot[:, 128:]) * scale


def solution(mesh):
    n, m = mesh.shape["items"], mesh.shape["users"]

    def body(user_emb, item_emb, target, history):
        u_dev, dsh = user_emb.shape
        item_dev, d = item_emb.shape
        half = u_dev // PARTS
        vmem = pl.BlockSpec(memory_space=pltpu.VMEM)
        smem = pl.BlockSpec(memory_space=pltpu.SMEM)
        hbm = pl.BlockSpec(memory_space=pltpu.HBM)
        dma = pltpu.SemaphoreType.DMA
        log_rank, metrics = pl.pallas_call(
            functools.partial(kernel, n, m),
            out_shape=(
                jax.ShapeDtypeStruct((1, u_dev), jnp.float32),
                jax.ShapeDtypeStruct((2,), jnp.float32),
            ),
            in_specs=[hbm, hbm, hbm, hbm],
            out_specs=(vmem, smem),
            scratch_shapes=[
                pltpu.VMEM((dsh, u_dev), jnp.bfloat16),
                pltpu.VMEM((1, u_dev), jnp.int32),
                pltpu.VMEM((history.shape[1], u_dev), jnp.int32),
                pltpu.SMEM((1, u_dev), jnp.int32),
                pltpu.SMEM((8, u_dev), jnp.int32),
                pltpu.VMEM((PARTS, n, dsh, half), jnp.bfloat16),
                pltpu.VMEM((d, u_dev), jnp.bfloat16),
                pltpu.VMEM((item_dev // TILE, TILE, d), jnp.bfloat16),
                pltpu.VMEM((u_dev, TILE, d), jnp.bfloat16),
                pltpu.VMEM((CHUNK, half), jnp.float32),
                pltpu.VMEM((CHUNK, half), jnp.float32),
                pltpu.VMEM((PARTS, 1, half), jnp.float32),
                pltpu.VMEM((PARTS, n, 1, half), jnp.float32),
                pltpu.VMEM((PARTS, 1, half), jnp.float32),
                pltpu.VMEM((PARTS, n, 1, half), jnp.float32),
                pltpu.VMEM((1, 256), jnp.float32),
                pltpu.VMEM((m, 1, 256), jnp.float32),
                pltpu.VMEM((1, u_dev), jnp.float32),
                dma((PIECES,)),
                dma((5,)),
                dma((PARTS, n - 1)), dma((PARTS, n - 1)),
                dma((PARTS, n - 1)), dma((PARTS, n - 1)),
                dma((PARTS, n - 1)), dma((PARTS, n - 1)),
                dma((m - 1,)), dma((m - 1,)),
            ],
            compiler_params=pltpu.CompilerParams(
                collective_id=0, has_side_effects=True, vmem_limit_bytes=60 << 20
            ),
        )(user_emb.T, item_emb.reshape(item_dev // TILE, TILE, d), target.reshape(1, u_dev), history.T)
        return log_rank.reshape(u_dev), metrics

    return jax.shard_map(
        body,
        mesh=mesh,
        in_specs=(P("users", "items"), P("items", None), P("users"), P("users", None)),
        out_specs=(P("users"), P()),
        check_vma=False,
    )
```

```python
import functools

import jax
import jax.numpy as jnp
from jax import lax
from jax.experimental import pallas as pl
from jax.experimental.pallas import tpu as pltpu
from jax.sharding import PartitionSpec as P

MESH = pl.DeviceIdType.MESH
CHUNK = 8192
PART = 256
PIECES = 8
BATCH = 16
TILE = 16


def exchange(axis, peers, src, dst, send, recv):
    return [
        pltpu.make_async_remote_copy(
            src_ref=src,
            dst_ref=dst,
            send_sem=send.at[i],
            recv_sem=recv.at[i],
            device_id={axis: peer},
            device_id_type=MESH,
        )
        for i, peer in enumerate(peers)
    ]


def start(copies):
    for c in copies:
        c.start()


def wait(copies):
    for c in copies:
        c.wait()


def collect(ids, items, rows):
    tiles = items.shape[0]

    def body(i, carry):
        some = rows.at[pl.ds(i * BATCH, BATCH)]
        for j in range(BATCH):
            some[j] = items[(ids[0, i * BATCH + j] >> 4) & (tiles - 1)]
        return carry

    lax.fori_loop(0, ids.shape[1] // BATCH, body, 0)


def own_scores(rows, w, ids, out):
    d = rows.shape[2]
    lane = lax.broadcasted_iota(jnp.int32, (TILE, 128), 1)
    sub = lax.broadcasted_iota(jnp.int32, (TILE, 128), 0)

    def body(i, carry):
        cols = pl.ds(pl.multiple_of(i * 128, 128), 128)
        pc = jnp.dot(rows[cols].reshape(128 * TILE, d), w[:, cols], preferred_element_type=jnp.float32)
        got = pc[:TILE]
        for r in range(1, 128):
            got = jnp.where(lane == r, pc[TILE * r : TILE * (r + 1)], got)
        here = sub == (ids[:, cols] & (TILE - 1))
        out[:, cols] = jnp.sum(jnp.where(here, got, 0.0), axis=0, keepdims=True)
        return carry

    return body


def kernel(
    n, m, u_hbm, item_ref, tgt_hbm, hist_hbm, out_ref,
    tgt_ref, hist_ref, tid_ref, hid_ref, gath0, gath1, w, items, trows, hrows, sa, sb,
    tdot, tpart0, tpart1, tslots0, tslots1, tsum_ref, hsc, apart0, apart1, aslots0, aslots1, mpart, mslots,
    sem_item, sem_in, us, ur, fs, fr, ts, tr, as_, ar, ms, mr,
):
    me = lax.axis_index("items")
    grp = lax.axis_index("users")
    chip, core = lax.div(me, 2), lax.rem(me, 2)
    dsh, u_dev = u_hbm.shape
    d = item_ref.shape[2]
    item_dev = item_ref.shape[0] * TILE
    piece = item_dev // TILE // PIECES
    parts = u_dev // PART
    steps = item_dev // CHUNK
    peers = [lax.rem(me + off, n) for off in range(1, n)]
    twins = [lax.rem(me + 2 * off, n) for off in range(1, n // 2)]
    mates = [lax.rem(grp + off, m) for off in range(1, m)]
    other = [me + 1 - 2 * core]

    ins = [
        pltpu.make_async_copy(u_hbm.at[:, :PART], gath0.at[core, chip], sem_in.at[0]),
        pltpu.make_async_copy(u_hbm.at[:, PART:], gath1.at[core, chip], sem_in.at[1]),
        pltpu.make_async_copy(tgt_hbm, tgt_ref, sem_in.at[2]),
        pltpu.make_async_copy(hist_hbm, hist_ref, sem_in.at[3]),
        pltpu.make_async_copy(tgt_hbm, tid_ref, sem_in.at[4]),
        pltpu.make_async_copy(hist_hbm.at[pl.ds(me, 1), :], hid_ref, sem_in.at[5]),
    ]
    start(ins)
    fetches = []
    for i in range(PIECES):
        part = pl.ds(i * piece, piece)
        fetches.append(pltpu.make_async_copy(item_ref.at[part], items.at[part], sem_item.at[i]))
    start(fetches)

    barrier = pltpu.get_barrier_semaphore()
    for peer in peers:
        pl.semaphore_signal(barrier, inc=1, device_id={"items": peer}, device_id_type=MESH)
    for peer in mates:
        pl.semaphore_signal(barrier, inc=1, device_id={"users": peer}, device_id_type=MESH)
    wait(ins)
    pl.semaphore_wait(barrier, n - 1 + m - 1)

    groups = ((0, 0, PART, gath0, tpart0, tslots0), (1, PART, u_dev, gath1, tpart1, tslots1))
    ucopies, fcopies, tcopies = [], [], []
    for g, lo, hi, gath, tpart, tslots in groups:
        mine = gath.at[core, chip]
        near = peers if g == 0 else twins
        ucopies.append(exchange("items", near, mine, mine, us.at[g], ur.at[g]))
        fcopies.append(exchange("items", other if g else [], gath.at[core], gath.at[core], fs.at[g], fr.at[g]))
        tcopies.append(exchange("items", peers, tpart, tslots.at[me], ts.at[g], tr.at[g]))
        start(ucopies[g])

    wait(fetches)
    collect(tid_ref, items, trows)
    collect(hid_ref, items, hrows)

    pick_target = own_scores(trows, w, tgt_ref, tdot)
    for g, lo, hi, gath, tpart, tslots in groups:
        wait(ucopies[g])
        start(fcopies[g])
        wait(fcopies[g])
        for i in range(n // 2):
            both = jnp.concatenate([gath[0, i], gath[1, i]], axis=0)
            w[2 * i * dsh : 2 * (i + 1) * dsh, lo:hi] = both * jnp.bfloat16(2)
        lax.fori_loop(lo // 128, hi // 128, pick_target, 0)
        local = tgt_ref[:, lo:hi] - me * item_dev
        tpart[...] = jnp.where((local >= 0) & (local < item_dev), tdot[:, lo:hi], 0.0)
        tslots[me] = tpart[...]
        start(tcopies[g])

    pick_history = own_scores(hrows, w, hist_ref.at[pl.ds(me, 1), :], hsc)

    def score(k, dst):
        at = lax.rem(k, steps) * (CHUNK // TILE)
        col = pl.multiple_of(lax.div(k, steps) * PART, PART)
        dst[...] = jnp.dot(
            items[pl.ds(at, CHUNK // TILE)].reshape(CHUNK, d), w[:, pl.ds(col, PART)], preferred_element_type=jnp.float32
        )

    def count(src, acc, t):
        sums = []
        for g in range(CHUNK // 8):
            v = jnp.tanh(src[8 * g : 8 * g + 8, :] - t) + 1.0
            lvl = 0
            while sums and sums[-1][0] == lvl and lvl < 3:
                v = sums.pop()[1] + v
                lvl += 1
            if lvl == 3:
                acc = acc + v
            else:
                sums.append((lvl, v))
        return acc

    def total(p):
        cols = pl.ds(pl.multiple_of(p * PART, PART), PART)
        tsum = tsum_ref[:, cols]
        t = jnp.broadcast_to(tsum, (8, PART))

        def step(i, acc):
            k = p * steps + 2 * i
            pick_history(p * (PART // 128) + i, 0)
            score(k + 1, sb)
            acc = count(sa, acc, t)
            score(lax.rem(k + 2, parts * steps), sa)
            return count(sb, acc, t)

        acc = lax.fori_loop(0, steps // 2, step, jnp.zeros((8, PART), jnp.float32))
        mine = jnp.tanh(hsc[:, cols] - tsum) + 1.0
        return 0.5 * (jnp.sum(acc, axis=0, keepdims=True) - mine)

    def add(slots):
        out = slots[0]
        for i in range(1, n):
            out = out + slots[i]
        return out

    acopies = [
        exchange("items", peers, apart0, aslots0.at[me], as_.at[0], ar.at[0]),
        exchange("items", peers, apart1, aslots1.at[me], as_.at[1], ar.at[1]),
    ]

    def each(p, carry):
        @pl.when(p == 1)
        def _():
            wait(tcopies[1])
            tsum_ref[:, PART:] = add(tslots1)

        got = total(p)

        @pl.when(p < parts - 1)
        def _():
            apart0[:, pl.ds(pl.multiple_of(p * PART, PART), PART)] = got

        @pl.when(p == parts - 2)
        def _():
            aslots0[me] = apart0[...]
            start(acopies[0])

        @pl.when(p == parts - 1)
        def _():
            apart1[...] = got
            aslots1[me] = got
            start(acopies[1])

        return carry

    score(0, sa)
    wait(tcopies[0])
    tsum_ref[:, :PART] = add(tslots0)
    lax.fori_loop(0, parts, each, 0)

    seen = jnp.max(jnp.where(hist_ref[...] == tgt_ref[...], 1.0, 0.0), axis=0, keepdims=True)
    hs = jnp.zeros((1, 128), jnp.float32)
    gs = jnp.zeros((1, 128), jnp.float32)
    for g, lo, hi, aslots in ((0, 0, u_dev - PART, aslots0), (1, u_dev - PART, u_dev, aslots1)):
        wait(acopies[g])
        rank = 1.0 + (add(aslots) - jnp.where(seen[:, lo:hi] > 0.5, 0.0, 0.5))
        out_ref[:, lo:hi] = jnp.log(rank)
        hit = jax.nn.sigmoid(10.5 - rank)
        gain = hit / jnp.log2(1.0 + rank)
        for b in range((hi - lo) // 128):
            hs = hs + hit[:, b * 128 : (b + 1) * 128]
            gs = gs + gain[:, b * 128 : (b + 1) * 128]
    mpart[:, :128] = hs
    mpart[:, 128:] = gs
    mslots[grp] = mpart[...]
    copies = exchange("users", mates, mpart, mslots.at[grp], ms, mr)
    start(copies)
    wait(copies)
    tot = mslots[0]
    for i in range(1, m):
        tot = tot + mslots[i]
    scale = 1.0 / (u_dev * m)
    hs = jnp.sum(tot[:, :128], axis=1, keepdims=True) * scale
    gs = jnp.sum(tot[:, 128:], axis=1, keepdims=True) * scale
    out_ref[:, u_dev:] = jnp.where(lax.broadcasted_iota(jnp.int32, (1, 128), 1) == 0, hs, gs)


def split(both, log_ref, met_ref):
    u_dev = log_ref.shape[0]
    log_ref[...] = both[0, :u_dev]
    met_ref[...] = both[0, u_dev : u_dev + 2]


def solution(mesh):
    n, m = mesh.shape["items"], mesh.shape["users"]

    def body(user_emb, item_emb, target, history):
        u_dev, dsh = user_emb.shape
        item_dev, d = item_emb.shape
        vmem = pl.BlockSpec(memory_space=pltpu.VMEM)
        hbm = pl.BlockSpec(memory_space=pltpu.HBM)
        dma = pltpu.SemaphoreType.DMA
        rest = u_dev - PART
        f32, bf16, i32 = jnp.float32, jnp.bfloat16, jnp.int32
        both = pl.pallas_call(
            functools.partial(kernel, n, m),
            out_shape=jax.ShapeDtypeStruct((1, u_dev + 128), f32),
            in_specs=[hbm, hbm, hbm, hbm],
            out_specs=vmem,
            scratch_shapes=[
                pltpu.VMEM((1, u_dev), i32),
                pltpu.VMEM((history.shape[1], u_dev), i32),
                pltpu.SMEM((1, u_dev), i32),
                pltpu.SMEM((1, u_dev), i32),
                pltpu.VMEM((2, n // 2, dsh, PART), bf16),
                pltpu.VMEM((2, n // 2, dsh, rest), bf16),
                pltpu.VMEM((d, u_dev), bf16),
                pltpu.VMEM((item_dev // TILE, TILE, d), bf16),
                pltpu.VMEM((u_dev, TILE, d), bf16),
                pltpu.VMEM((u_dev, TILE, d), bf16),
                pltpu.VMEM((CHUNK, PART), f32),
                pltpu.VMEM((CHUNK, PART), f32),
                pltpu.VMEM((1, u_dev), f32),
                pltpu.VMEM((1, PART), f32),
                pltpu.VMEM((1, rest), f32),
                pltpu.VMEM((n, 1, PART), f32),
                pltpu.VMEM((n, 1, rest), f32),
                pltpu.VMEM((1, u_dev), f32),
                pltpu.VMEM((1, u_dev), f32),
                pltpu.VMEM((1, rest), f32),
                pltpu.VMEM((1, PART), f32),
                pltpu.VMEM((n, 1, rest), f32),
                pltpu.VMEM((n, 1, PART), f32),
                pltpu.VMEM((1, 256), f32),
                pltpu.VMEM((m, 1, 256), f32),
                dma((PIECES,)),
                dma((6,)),
                dma((2, n - 1)), dma((2, n - 1)),
                dma((2, 1)), dma((2, 1)),
                dma((2, n - 1)), dma((2, n - 1)),
                dma((2, n - 1)), dma((2, n - 1)),
                dma((m - 1,)), dma((m - 1,)),
            ],
            compiler_params=pltpu.CompilerParams(
                collective_id=0, has_side_effects=True, vmem_limit_bytes=60 << 20
            ),
        )(user_emb.T, item_emb.reshape(item_dev // TILE, TILE, d), target.reshape(1, u_dev), history.T)
        return pl.pallas_call(
            split,
            out_shape=(jax.ShapeDtypeStruct((u_dev,), f32), jax.ShapeDtypeStruct((2,), f32)),
            in_specs=[vmem],
            out_specs=(vmem, vmem),
        )(both)

    return jax.shard_map(
        body,
        mesh=mesh,
        in_specs=(P("users", "items"), P("items", None), P("users"), P("users", None)),
        out_specs=(P("users"), P()),
        check_vma=False,
    )
```

```python
import functools

import jax
import jax.numpy as jnp
from jax import lax
from jax.experimental import pallas as pl
from jax.experimental.pallas import tpu as pltpu
from jax.sharding import PartitionSpec as P

MESH = pl.DeviceIdType.MESH
CHUNK = 8192
PART = 256
PIECES = 8
BATCH = 32
TILE = 8


def exchange(axis, peers, src, dst, send, recv):
    return [
        pltpu.make_async_remote_copy(
            src_ref=src,
            dst_ref=dst,
            send_sem=send.at[i],
            recv_sem=recv.at[i],
            device_id={axis: peer},
            device_id_type=MESH,
        )
        for i, peer in enumerate(peers)
    ]


def start(copies):
    for c in copies:
        c.start()


def wait(copies):
    for c in copies:
        c.wait()


def collect(ids, items, rows):
    tiles = items.shape[0]

    def body(i, carry):
        some = rows.at[pl.ds(i * BATCH, BATCH)]
        for j in range(BATCH):
            some[j] = items[(ids[0, i * BATCH + j] >> 3) & (tiles - 1)]
        return carry

    lax.fori_loop(0, ids.shape[1] // BATCH, body, 0)


def own_scores(rows, w, ids, out):
    d = rows.shape[2]
    lane = lax.broadcasted_iota(jnp.int32, (TILE, 128), 1)
    sub = lax.broadcasted_iota(jnp.int32, (TILE, 128), 0)

    def body(i, carry):
        cols = pl.ds(pl.multiple_of(i * 128, 128), 128)
        pc = jnp.dot(rows[cols].reshape(128 * TILE, d), w[:, cols], preferred_element_type=jnp.float32)
        got = pc[:TILE]
        for r in range(1, 128):
            got = jnp.where(lane == r, pc[TILE * r : TILE * (r + 1)], got)
        here = sub == (ids[:, cols] & (TILE - 1))
        out[:, cols] = jnp.sum(jnp.where(here, got, 0.0), axis=0, keepdims=True)
        return carry

    return body


def kernel(
    n, m, u_hbm, item_ref, tgt_hbm, hist_hbm, out_ref,
    tgt_ref, hist_ref, tid_ref, hid_ref, gath0, gath1, w, items, trows, hrows, sa, sb,
    tdot, tpart0, tpart1, tslots0, tslots1, tsum_ref, hsc, apart0, apart1, aslots0, aslots1, mpart, mslots,
    sem_item, sem_in, us, ur, fs, fr, ts, tr, as_, ar, ms, mr,
):
    me = lax.axis_index("items")
    grp = lax.axis_index("users")
    chip, core = lax.div(me, 2), lax.rem(me, 2)
    dsh, u_dev = u_hbm.shape
    d = item_ref.shape[2]
    item_dev = item_ref.shape[0] * TILE
    piece = item_dev // TILE // PIECES
    parts = u_dev // PART
    steps = item_dev // CHUNK
    peers = [lax.rem(me + off, n) for off in range(1, n)]
    twins = [lax.rem(me + 2 * off, n) for off in range(1, n // 2)]
    mates = [lax.rem(grp + off, m) for off in range(1, m)]
    other = [me + 1 - 2 * core]

    ins = [
        pltpu.make_async_copy(u_hbm.at[:, :PART], gath0.at[core, chip], sem_in.at[0]),
        pltpu.make_async_copy(u_hbm.at[:, PART:], gath1.at[core, chip], sem_in.at[1]),
        pltpu.make_async_copy(tgt_hbm, tgt_ref, sem_in.at[2]),
        pltpu.make_async_copy(hist_hbm, hist_ref, sem_in.at[3]),
        pltpu.make_async_copy(tgt_hbm, tid_ref, sem_in.at[4]),
        pltpu.make_async_copy(hist_hbm.at[pl.ds(me, 1), :], hid_ref, sem_in.at[5]),
    ]
    start(ins)
    fetches = []
    for i in range(PIECES):
        part = pl.ds(i * piece, piece)
        fetches.append(pltpu.make_async_copy(item_ref.at[part], items.at[part], sem_item.at[i]))
    start(fetches)

    barrier = pltpu.get_barrier_semaphore()
    for peer in peers:
        pl.semaphore_signal(barrier, inc=1, device_id={"items": peer}, device_id_type=MESH)
    for peer in mates:
        pl.semaphore_signal(barrier, inc=1, device_id={"users": peer}, device_id_type=MESH)
    wait(ins)
    pl.semaphore_wait(barrier, n - 1 + m - 1)

    groups = ((0, 0, PART, gath0, tpart0, tslots0), (1, PART, u_dev, gath1, tpart1, tslots1))
    ucopies, fcopies, tcopies = [], [], []
    for g, lo, hi, gath, tpart, tslots in groups:
        mine = gath.at[core, chip]
        near = peers if g == 0 else twins
        ucopies.append(exchange("items", near, mine, mine, us.at[g], ur.at[g]))
        fcopies.append(exchange("items", other if g else [], gath.at[core], gath.at[core], fs.at[g], fr.at[g]))
        tcopies.append(exchange("items", peers, tpart, tslots.at[me], ts.at[g], tr.at[g]))
        start(ucopies[g])

    wait(fetches)
    collect(tid_ref, items, trows)

    def score(k, dst):
        at = lax.rem(k, steps) * (CHUNK // TILE)
        col = pl.multiple_of(lax.div(k, steps) * PART, PART)
        dst[...] = jnp.dot(
            items[pl.ds(at, CHUNK // TILE)].reshape(CHUNK, d), w[:, pl.ds(col, PART)], preferred_element_type=jnp.float32
        )

    pick_target = own_scores(trows, w, tgt_ref, tdot)
    for g, lo, hi, gath, tpart, tslots in groups:
        wait(ucopies[g])
        start(fcopies[g])
        if g == 1:
            score(0, sa)
        wait(fcopies[g])
        for i in range(n // 2):
            both = jnp.concatenate([gath[0, i], gath[1, i]], axis=0)
            w[2 * i * dsh : 2 * (i + 1) * dsh, lo:hi] = both * jnp.bfloat16(2)
        lax.fori_loop(lo // 128, hi // 128, pick_target, 0)
        local = tgt_ref[:, lo:hi] - me * item_dev
        tpart[...] = jnp.where((local >= 0) & (local < item_dev), tdot[:, lo:hi], 0.0)
        tslots[me] = tpart[...]
        start(tcopies[g])
        if g == 0:
            collect(hid_ref, items, hrows)

    pick_history = own_scores(hrows, w, hist_ref.at[pl.ds(me, 1), :], hsc)

    def count(src, acc, t):
        sums = []
        for g in range(CHUNK // 8):
            v = jnp.tanh(src[8 * g : 8 * g + 8, :] - t) + 1.0
            lvl = 0
            while sums and sums[-1][0] == lvl and lvl < 3:
                v = sums.pop()[1] + v
                lvl += 1
            if lvl == 3:
                acc = acc + v
            else:
                sums.append((lvl, v))
        return acc

    def total(p):
        cols = pl.ds(pl.multiple_of(p * PART, PART), PART)
        tsum = tsum_ref[:, cols]
        t = jnp.broadcast_to(tsum, (8, PART))

        def step(i, acc):
            k = p * steps + 2 * i
            pick_history(p * (PART // 128) + i, 0)
            score(k + 1, sb)
            acc = count(sa, acc, t)
            score(lax.rem(k + 2, parts * steps), sa)
            return count(sb, acc, t)

        acc = lax.fori_loop(0, steps // 2, step, jnp.zeros((8, PART), jnp.float32))
        mine = jnp.tanh(hsc[:, cols] - tsum) + 1.0
        return 0.5 * (jnp.sum(acc, axis=0, keepdims=True) - mine)

    def add(slots):
        out = slots[0]
        for i in range(1, n):
            out = out + slots[i]
        return out

    acopies = [
        exchange("items", peers, apart0, aslots0.at[me], as_.at[0], ar.at[0]),
        exchange("items", peers, apart1, aslots1.at[me], as_.at[1], ar.at[1]),
    ]

    def each(p, carry):
        @pl.when(p == 1)
        def _():
            wait(tcopies[1])
            tsum_ref[:, PART:] = add(tslots1)

        got = total(p)

        @pl.when(p < parts - 1)
        def _():
            apart0[:, pl.ds(pl.multiple_of(p * PART, PART), PART)] = got

        @pl.when(p == parts - 2)
        def _():
            aslots0[me] = apart0[...]
            start(acopies[0])

        @pl.when(p == parts - 1)
        def _():
            apart1[...] = got
            aslots1[me] = got
            start(acopies[1])

        return carry

    wait(tcopies[0])
    tsum_ref[:, :PART] = add(tslots0)
    lax.fori_loop(0, parts, each, 0)

    seen = jnp.max(jnp.where(hist_ref[...] == tgt_ref[...], 1.0, 0.0), axis=0, keepdims=True)
    hs = jnp.zeros((1, 128), jnp.float32)
    gs = jnp.zeros((1, 128), jnp.float32)
    for g, lo, hi, aslots in ((0, 0, u_dev - PART, aslots0), (1, u_dev - PART, u_dev, aslots1)):
        wait(acopies[g])
        rank = 1.0 + (add(aslots) - jnp.where(seen[:, lo:hi] > 0.5, 0.0, 0.5))
        out_ref[:, lo:hi] = jnp.log(rank)
        hit = jax.nn.sigmoid(10.5 - rank)
        gain = hit / jnp.log2(1.0 + rank)
        for b in range((hi - lo) // 128):
            hs = hs + hit[:, b * 128 : (b + 1) * 128]
            gs = gs + gain[:, b * 128 : (b + 1) * 128]
    mpart[:, :128] = hs
    mpart[:, 128:] = gs
    mslots[grp] = mpart[...]
    copies = exchange("users", mates, mpart, mslots.at[grp], ms, mr)
    start(copies)
    wait(copies)
    tot = mslots[0]
    for i in range(1, m):
        tot = tot + mslots[i]
    scale = 1.0 / (u_dev * m)
    hs = jnp.sum(tot[:, :128], axis=1, keepdims=True) * scale
    gs = jnp.sum(tot[:, 128:], axis=1, keepdims=True) * scale
    out_ref[:, u_dev:] = jnp.where(lax.broadcasted_iota(jnp.int32, (1, 128), 1) == 0, hs, gs)


def split(both, log_ref, met_ref):
    u_dev = log_ref.shape[0]
    log_ref[...] = both[0, :u_dev]
    met_ref[...] = both[0, u_dev : u_dev + 2]


def solution(mesh):
    n, m = mesh.shape["items"], mesh.shape["users"]

    def body(user_emb, item_emb, target, history):
        u_dev, dsh = user_emb.shape
        item_dev, d = item_emb.shape
        vmem = pl.BlockSpec(memory_space=pltpu.VMEM)
        hbm = pl.BlockSpec(memory_space=pltpu.HBM)
        dma = pltpu.SemaphoreType.DMA
        rest = u_dev - PART
        f32, bf16, i32 = jnp.float32, jnp.bfloat16, jnp.int32
        both = pl.pallas_call(
            functools.partial(kernel, n, m),
            out_shape=jax.ShapeDtypeStruct((1, u_dev + 128), f32),
            in_specs=[hbm, hbm, hbm, hbm],
            out_specs=vmem,
            scratch_shapes=[
                pltpu.VMEM((1, u_dev), i32),
                pltpu.VMEM((history.shape[1], u_dev), i32),
                pltpu.SMEM((1, u_dev), i32),
                pltpu.SMEM((1, u_dev), i32),
                pltpu.VMEM((2, n // 2, dsh, PART), bf16),
                pltpu.VMEM((2, n // 2, dsh, rest), bf16),
                pltpu.VMEM((d, u_dev), bf16),
                pltpu.VMEM((item_dev // TILE, TILE, d), bf16),
                pltpu.VMEM((u_dev, TILE, d), bf16),
                pltpu.VMEM((u_dev, TILE, d), bf16),
                pltpu.VMEM((CHUNK, PART), f32),
                pltpu.VMEM((CHUNK, PART), f32),
                pltpu.VMEM((1, u_dev), f32),
                pltpu.VMEM((1, PART), f32),
                pltpu.VMEM((1, rest), f32),
                pltpu.VMEM((n, 1, PART), f32),
                pltpu.VMEM((n, 1, rest), f32),
                pltpu.VMEM((1, u_dev), f32),
                pltpu.VMEM((1, u_dev), f32),
                pltpu.VMEM((1, rest), f32),
                pltpu.VMEM((1, PART), f32),
                pltpu.VMEM((n, 1, rest), f32),
                pltpu.VMEM((n, 1, PART), f32),
                pltpu.VMEM((1, 256), f32),
                pltpu.VMEM((m, 1, 256), f32),
                dma((PIECES,)),
                dma((6,)),
                dma((2, n - 1)), dma((2, n - 1)),
                dma((2, 1)), dma((2, 1)),
                dma((2, n - 1)), dma((2, n - 1)),
                dma((2, n - 1)), dma((2, n - 1)),
                dma((m - 1,)), dma((m - 1,)),
            ],
            compiler_params=pltpu.CompilerParams(
                collective_id=0, has_side_effects=True, vmem_limit_bytes=60 << 20
            ),
        )(user_emb.T, item_emb.reshape(item_dev // TILE, TILE, d), target.reshape(1, u_dev), history.T)
        return pl.pallas_call(
            split,
            out_shape=(jax.ShapeDtypeStruct((u_dev,), f32), jax.ShapeDtypeStruct((2,), f32)),
            in_specs=[vmem],
            out_specs=(vmem, vmem),
        )(both)

    return jax.shard_map(
        body,
        mesh=mesh,
        in_specs=(P("users", "items"), P("items", None), P("users"), P("users", None)),
        out_specs=(P("users"), P()),
        check_vma=False,
    )
```

```python
import functools

import jax
import jax.numpy as jnp
from jax import lax
from jax.experimental import pallas as pl
from jax.experimental.pallas import tpu as pltpu
from jax.sharding import PartitionSpec as P

MESH = pl.DeviceIdType.MESH
CHUNK = 8192
PART = 256
PIECES = 8
BATCH = 32
TILE = 8


def exchange(axis, peers, src, dst, send, recv):
    return [
        pltpu.make_async_remote_copy(
            src_ref=src,
            dst_ref=dst,
            send_sem=send.at[i],
            recv_sem=recv.at[i],
            device_id={axis: peer},
            device_id_type=MESH,
        )
        for i, peer in enumerate(peers)
    ]


def start(copies):
    for c in copies:
        c.start()


def wait(copies):
    for c in copies:
        c.wait()


def collect(ids, items, rows):
    tiles = items.shape[0]

    def body(i, carry):
        some = rows.at[pl.ds(i * BATCH, BATCH)]
        for j in range(BATCH):
            some[j] = items[(ids[0, i * BATCH + j] >> 3) & (tiles - 1)]
        return carry

    lax.fori_loop(0, ids.shape[1] // BATCH, body, 0)


def own_scores(rows, w, ids, out):
    d = rows.shape[2]
    lane = lax.broadcasted_iota(jnp.int32, (TILE, 128), 1)
    sub = lax.broadcasted_iota(jnp.int32, (TILE, 128), 0)

    def body(i, carry):
        cols = pl.ds(pl.multiple_of(i * 128, 128), 128)
        pc = jnp.dot(rows[cols].reshape(128 * TILE, d), w[:, cols], preferred_element_type=jnp.float32)
        got = pc[:TILE]
        for r in range(1, 128):
            got = jnp.where(lane == r, pc[TILE * r : TILE * (r + 1)], got)
        here = sub == (ids[:, cols] & (TILE - 1))
        out[:, cols] = jnp.sum(jnp.where(here, got, 0.0), axis=0, keepdims=True)
        return carry

    return body


def kernel(
    n, m, u_hbm, item_ref, tgt_hbm, hist_hbm, out_ref,
    tgt_ref, hist_ref, tid_ref, hid_ref, gath0, gath1, w, items, trows, hrows, sa, sb,
    tdot, tpart0, tpart1, tslots0, tslots1, tsum_ref, hsc, apart0, apart1, aslots0, aslots1, mpart, mslots,
    sem_item, sem_in, us, ur, fs, fr, ts, tr, as_, ar, ms, mr,
):
    me = lax.axis_index("items")
    grp = lax.axis_index("users")
    chip, core = lax.div(me, 2), lax.rem(me, 2)
    dsh, u_dev = u_hbm.shape
    d = item_ref.shape[2]
    item_dev = item_ref.shape[0] * TILE
    piece = item_dev // TILE // PIECES
    parts = u_dev // PART
    steps = item_dev // CHUNK
    peers = [lax.rem(me + off, n) for off in range(1, n)]
    twins = [lax.rem(me + 2 * off, n) for off in range(1, n // 2)]
    mates = [lax.rem(grp + off, m) for off in range(1, m)]
    other = [me + 1 - 2 * core]

    ins = [
        pltpu.make_async_copy(u_hbm.at[:, :PART], gath0.at[core, chip], sem_in.at[0]),
        pltpu.make_async_copy(u_hbm.at[:, PART:], gath1.at[core, chip], sem_in.at[1]),
        pltpu.make_async_copy(tgt_hbm, tgt_ref, sem_in.at[2]),
        pltpu.make_async_copy(hist_hbm, hist_ref, sem_in.at[3]),
        pltpu.make_async_copy(tgt_hbm, tid_ref, sem_in.at[4]),
        pltpu.make_async_copy(hist_hbm.at[pl.ds(me, 1), :], hid_ref, sem_in.at[5]),
    ]
    start(ins)
    fetches = []
    for i in range(PIECES):
        part = pl.ds(i * piece, piece)
        fetches.append(pltpu.make_async_copy(item_ref.at[part], items.at[part], sem_item.at[i]))
    start(fetches)

    barrier = pltpu.get_barrier_semaphore()
    for peer in peers:
        pl.semaphore_signal(barrier, inc=1, device_id={"items": peer}, device_id_type=MESH)
    for peer in mates:
        pl.semaphore_signal(barrier, inc=1, device_id={"users": peer}, device_id_type=MESH)
    wait(ins)
    pl.semaphore_wait(barrier, n - 1 + m - 1)

    groups = ((0, 0, PART, gath0, tpart0, tslots0), (1, PART, u_dev, gath1, tpart1, tslots1))
    ucopies, fcopies, tcopies = [], [], []
    for g, lo, hi, gath, tpart, tslots in groups:
        mine = gath.at[core, chip]
        near = peers if g == 0 else twins
        ucopies.append(exchange("items", near, mine, mine, us.at[g], ur.at[g]))
        fcopies.append(exchange("items", other if g else [], gath.at[core], gath.at[core], fs.at[g], fr.at[g]))
        tcopies.append(exchange("items", peers, tpart, tslots.at[me], ts.at[g], tr.at[g]))
        start(ucopies[g])

    wait(fetches)
    collect(tid_ref, items, trows)

    def score(k, dst):
        at = lax.rem(k, steps) * (CHUNK // TILE)
        col = pl.multiple_of(lax.div(k, steps) * PART, PART)
        dst[...] = jnp.dot(
            items[pl.ds(at, CHUNK // TILE)].reshape(CHUNK, d), w[:, pl.ds(col, PART)], preferred_element_type=jnp.float32
        )

    pick_target = own_scores(trows, w, tgt_ref, tdot)

    def pick_part(i, carry):
        for b in range(PART // 128):
            carry = pick_target(i * (PART // 128) + b, carry)
        return carry

    for g, lo, hi, gath, tpart, tslots in groups:
        wait(ucopies[g])
        start(fcopies[g])
        if g == 1:
            score(0, sa)
        wait(fcopies[g])
        for i in range(n // 2):
            both = jnp.concatenate([gath[0, i], gath[1, i]], axis=0)
            w[2 * i * dsh : 2 * (i + 1) * dsh, lo:hi] = both * jnp.bfloat16(2)
        lax.fori_loop(lo // PART, hi // PART, pick_part, 0)
        local = tgt_ref[:, lo:hi] - me * item_dev
        tpart[...] = jnp.where((local >= 0) & (local < item_dev), tdot[:, lo:hi], 0.0)
        tslots[me] = tpart[...]
        start(tcopies[g])
        if g == 0:
            collect(hid_ref, items, hrows)

    pick_history = own_scores(hrows, w, hist_ref.at[pl.ds(me, 1), :], hsc)

    def count(src, acc, t):
        sums = []
        for g in range(CHUNK // 8):
            v = jnp.tanh(src[8 * g : 8 * g + 8, :] - t) + 1.0
            lvl = 0
            while sums and sums[-1][0] == lvl and lvl < 3:
                v = sums.pop()[1] + v
                lvl += 1
            if lvl == 3:
                acc = acc + v
            else:
                sums.append((lvl, v))
        return acc

    def total(p):
        cols = pl.ds(pl.multiple_of(p * PART, PART), PART)
        tsum = tsum_ref[:, cols]
        t = jnp.broadcast_to(tsum, (8, PART))

        def step(i, acc):
            k = p * steps + 2 * i
            score(k + 1, sb)
            acc = count(sa, acc, t)
            pick_history(p * (PART // 128) + i, 0)
            score(lax.rem(k + 2, parts * steps), sa)
            return count(sb, acc, t)

        acc = lax.fori_loop(0, steps // 2, step, jnp.zeros((8, PART), jnp.float32))
        mine = jnp.tanh(hsc[:, cols] - tsum) + 1.0
        return 0.5 * (jnp.sum(acc, axis=0, keepdims=True) - mine)

    def add(slots):
        out = slots[0]
        for i in range(1, n):
            out = out + slots[i]
        return out

    acopies = [
        exchange("items", peers, apart0, aslots0.at[me], as_.at[0], ar.at[0]),
        exchange("items", peers, apart1, aslots1.at[me], as_.at[1], ar.at[1]),
    ]

    def each(p, carry):
        @pl.when(p == 1)
        def _():
            wait(tcopies[1])
            tsum_ref[:, PART:] = add(tslots1)

        got = total(p)

        @pl.when(p < parts - 1)
        def _():
            apart0[:, pl.ds(pl.multiple_of(p * PART, PART), PART)] = got

        @pl.when(p == parts - 2)
        def _():
            aslots0[me] = apart0[...]
            start(acopies[0])

        @pl.when(p == parts - 1)
        def _():
            apart1[...] = got
            aslots1[me] = got
            start(acopies[1])

        return carry

    wait(tcopies[0])
    tsum_ref[:, :PART] = add(tslots0)
    lax.fori_loop(0, parts, each, 0)

    seen = jnp.max(jnp.where(hist_ref[...] == tgt_ref[...], 1.0, 0.0), axis=0, keepdims=True)
    hs = jnp.zeros((1, 128), jnp.float32)
    gs = jnp.zeros((1, 128), jnp.float32)
    for g, lo, hi, aslots in ((0, 0, u_dev - PART, aslots0), (1, u_dev - PART, u_dev, aslots1)):
        wait(acopies[g])
        rank = 1.0 + (add(aslots) - jnp.where(seen[:, lo:hi] > 0.5, 0.0, 0.5))
        out_ref[:, lo:hi] = jnp.log(rank)
        hit = jax.nn.sigmoid(10.5 - rank)
        gain = hit / jnp.log2(1.0 + rank)
        for b in range((hi - lo) // 128):
            hs = hs + hit[:, b * 128 : (b + 1) * 128]
            gs = gs + gain[:, b * 128 : (b + 1) * 128]
    mpart[:, :128] = hs
    mpart[:, 128:] = gs
    mslots[grp] = mpart[...]
    copies = exchange("users", mates, mpart, mslots.at[grp], ms, mr)
    start(copies)
    wait(copies)
    tot = mslots[0]
    for i in range(1, m):
        tot = tot + mslots[i]
    scale = 1.0 / (u_dev * m)
    hs = jnp.sum(tot[:, :128], axis=1, keepdims=True) * scale
    gs = jnp.sum(tot[:, 128:], axis=1, keepdims=True) * scale
    out_ref[:, u_dev:] = jnp.where(lax.broadcasted_iota(jnp.int32, (1, 128), 1) == 0, hs, gs)


def split(both, log_ref, met_ref):
    u_dev = log_ref.shape[0]
    log_ref[...] = both[0, :u_dev]
    met_ref[...] = both[0, u_dev : u_dev + 2]


def solution(mesh):
    n, m = mesh.shape["items"], mesh.shape["users"]

    def body(user_emb, item_emb, target, history):
        u_dev, dsh = user_emb.shape
        item_dev, d = item_emb.shape
        vmem = pl.BlockSpec(memory_space=pltpu.VMEM)
        hbm = pl.BlockSpec(memory_space=pltpu.HBM)
        dma = pltpu.SemaphoreType.DMA
        rest = u_dev - PART
        f32, bf16, i32 = jnp.float32, jnp.bfloat16, jnp.int32
        both = pl.pallas_call(
            functools.partial(kernel, n, m),
            out_shape=jax.ShapeDtypeStruct((1, u_dev + 128), f32),
            in_specs=[hbm, hbm, hbm, hbm],
            out_specs=vmem,
            scratch_shapes=[
                pltpu.VMEM((1, u_dev), i32),
                pltpu.VMEM((history.shape[1], u_dev), i32),
                pltpu.SMEM((1, u_dev), i32),
                pltpu.SMEM((1, u_dev), i32),
                pltpu.VMEM((2, n // 2, dsh, PART), bf16),
                pltpu.VMEM((2, n // 2, dsh, rest), bf16),
                pltpu.VMEM((d, u_dev), bf16),
                pltpu.VMEM((item_dev // TILE, TILE, d), bf16),
                pltpu.VMEM((u_dev, TILE, d), bf16),
                pltpu.VMEM((u_dev, TILE, d), bf16),
                pltpu.VMEM((CHUNK, PART), f32),
                pltpu.VMEM((CHUNK, PART), f32),
                pltpu.VMEM((1, u_dev), f32),
                pltpu.VMEM((1, PART), f32),
                pltpu.VMEM((1, rest), f32),
                pltpu.VMEM((n, 1, PART), f32),
                pltpu.VMEM((n, 1, rest), f32),
                pltpu.VMEM((1, u_dev), f32),
                pltpu.VMEM((1, u_dev), f32),
                pltpu.VMEM((1, rest), f32),
                pltpu.VMEM((1, PART), f32),
                pltpu.VMEM((n, 1, rest), f32),
                pltpu.VMEM((n, 1, PART), f32),
                pltpu.VMEM((1, 256), f32),
                pltpu.VMEM((m, 1, 256), f32),
                dma((PIECES,)),
                dma((6,)),
                dma((2, n - 1)), dma((2, n - 1)),
                dma((2, 1)), dma((2, 1)),
                dma((2, n - 1)), dma((2, n - 1)),
                dma((2, n - 1)), dma((2, n - 1)),
                dma((m - 1,)), dma((m - 1,)),
            ],
            compiler_params=pltpu.CompilerParams(
                collective_id=0, has_side_effects=True, vmem_limit_bytes=60 << 20
            ),
        )(user_emb.T, item_emb.reshape(item_dev // TILE, TILE, d), target.reshape(1, u_dev), history.T)
        return pl.pallas_call(
            split,
            out_shape=(jax.ShapeDtypeStruct((u_dev,), f32), jax.ShapeDtypeStruct((2,), f32)),
            in_specs=[vmem],
            out_specs=(vmem, vmem),
        )(both)

    return jax.shard_map(
        body,
        mesh=mesh,
        in_specs=(P("users", "items"), P("items", None), P("users"), P("users", None)),
        out_specs=(P("users"), P()),
        check_vma=False,
    )
```

```python
import functools

import jax
import jax.numpy as jnp
from jax import lax
from jax.experimental import pallas as pl
from jax.experimental.pallas import tpu as pltpu
from jax.sharding import PartitionSpec as P

MESH = pl.DeviceIdType.MESH
CHUNK = 8192
PART = 256
PIECES = 8
BATCH = 32
TILE = 8


def exchange(axis, peers, src, dst, send, recv):
    return [
        pltpu.make_async_remote_copy(
            src_ref=src,
            dst_ref=dst,
            send_sem=send.at[i],
            recv_sem=recv.at[i],
            device_id={axis: peer},
            device_id_type=MESH,
        )
        for i, peer in enumerate(peers)
    ]


def start(copies):
    for c in copies:
        c.start()


def wait(copies):
    for c in copies:
        c.wait()


def collect(ids, items, rows):
    tiles = items.shape[0]

    def body(i, carry):
        some = rows.at[pl.ds(i * BATCH, BATCH)]
        for j in range(BATCH):
            some[j] = items[(ids[0, i * BATCH + j] >> 3) & (tiles - 1)]
        return carry

    lax.fori_loop(0, ids.shape[1] // BATCH, body, 0)


def own_scores(rows, w, ids, out):
    d = rows.shape[2]
    lane = lax.broadcasted_iota(jnp.int32, (TILE, 128), 1)
    sub = lax.broadcasted_iota(jnp.int32, (TILE, 128), 0)

    def body(i, carry):
        cols = pl.ds(pl.multiple_of(i * 128, 128), 128)
        pc = jnp.dot(rows[cols].reshape(128 * TILE, d), w[:, cols], preferred_element_type=jnp.float32)
        got = pc[:TILE]
        for r in range(1, 128):
            got = jnp.where(lane == r, pc[TILE * r : TILE * (r + 1)], got)
        here = sub == (ids[:, cols] & (TILE - 1))
        out[:, cols] = jnp.sum(jnp.where(here, got, 0.0), axis=0, keepdims=True)
        return carry

    return body


def kernel(
    n, m, u_hbm, item_ref, tgt_hbm, hist_hbm, out_ref,
    tgt_ref, hist_ref, tid_ref, hid_ref, gath0, gath1, w, items, trows, hrows, sa, sb,
    tdot, tpart0, tpart1, tslots0, tslots1, tsum_ref, hsc, apart0, apart1, aslots0, aslots1, mpart, mslots,
    sem_item, sem_in, us, ur, fs, fr, ts, tr, as_, ar, ms, mr,
):
    me = lax.axis_index("items")
    grp = lax.axis_index("users")
    chip, core = lax.div(me, 2), lax.rem(me, 2)
    dsh, u_dev = u_hbm.shape
    d = item_ref.shape[2]
    item_dev = item_ref.shape[0] * TILE
    piece = item_dev // TILE // PIECES
    parts = u_dev // PART
    steps = item_dev // CHUNK
    peers = [lax.rem(me + off, n) for off in range(1, n)]
    twins = [lax.rem(me + 2 * off, n) for off in range(1, n // 2)]
    mates = [lax.rem(grp + off, m) for off in range(1, m)]
    other = [me + 1 - 2 * core]

    ins = [
        pltpu.make_async_copy(u_hbm.at[:, :PART], gath0.at[core, chip], sem_in.at[0]),
        pltpu.make_async_copy(u_hbm.at[:, PART:], gath1.at[core, chip], sem_in.at[1]),
        pltpu.make_async_copy(tgt_hbm, tgt_ref, sem_in.at[2]),
        pltpu.make_async_copy(hist_hbm, hist_ref, sem_in.at[3]),
        pltpu.make_async_copy(tgt_hbm, tid_ref, sem_in.at[4]),
        pltpu.make_async_copy(hist_hbm.at[pl.ds(me, 1), :], hid_ref, sem_in.at[5]),
    ]
    start(ins)
    fetches = []
    for i in range(PIECES):
        part = pl.ds(i * piece, piece)
        fetches.append(pltpu.make_async_copy(item_ref.at[part], items.at[part], sem_item.at[i]))
    start(fetches)

    barrier = pltpu.get_barrier_semaphore()
    for peer in peers:
        pl.semaphore_signal(barrier, inc=1, device_id={"items": peer}, device_id_type=MESH)
    for peer in mates:
        pl.semaphore_signal(barrier, inc=1, device_id={"users": peer}, device_id_type=MESH)
    wait(ins)
    pl.semaphore_wait(barrier, n - 1 + m - 1)

    groups = ((0, 0, PART, gath0, tpart0, tslots0), (1, PART, u_dev, gath1, tpart1, tslots1))
    ucopies, fcopies, tcopies = [], [], []
    for g, lo, hi, gath, tpart, tslots in groups:
        mine = gath.at[core, chip]
        near = peers if g == 0 else twins
        ucopies.append(exchange("items", near, mine, mine, us.at[g], ur.at[g]))
        fcopies.append(exchange("items", other if g else [], gath.at[core], gath.at[core], fs.at[g], fr.at[g]))
        tcopies.append(exchange("items", peers, tpart, tslots.at[me], ts.at[g], tr.at[g]))
        start(ucopies[g])

    wait(fetches)
    collect(tid_ref, items, trows)
    collect(hid_ref, items, hrows)

    def score(k, dst):
        at = lax.rem(k, steps) * (CHUNK // TILE)
        col = pl.multiple_of(lax.div(k, steps) * PART, PART)
        dst[...] = jnp.dot(
            items[pl.ds(at, CHUNK // TILE)].reshape(CHUNK, d), w[:, pl.ds(col, PART)], preferred_element_type=jnp.float32
        )

    pick_target = own_scores(trows, w, tgt_ref, tdot)

    for g, lo, hi, gath, tpart, tslots in groups:
        wait(ucopies[g])
        start(fcopies[g])
        if g == 1:
            score(0, sa)
        wait(fcopies[g])
        for i in range(n // 2):
            both = jnp.concatenate([gath[0, i], gath[1, i]], axis=0)
            w[2 * i * dsh : 2 * (i + 1) * dsh, lo:hi] = both * jnp.bfloat16(2)
        per = 2 if g == 0 else 3

        def pick_some(i, carry, first=lo // 128, per=per):
            for b in range(per):
                carry = pick_target(first + i * per + b, carry)
            return carry

        lax.fori_loop(0, (hi - lo) // 128 // per, pick_some, 0)
        local = tgt_ref[:, lo:hi] - me * item_dev
        tpart[...] = jnp.where((local >= 0) & (local < item_dev), tdot[:, lo:hi], 0.0)
        tslots[me] = tpart[...]
        start(tcopies[g])

    pick_history = own_scores(hrows, w, hist_ref.at[pl.ds(me, 1), :], hsc)

    def count(src, acc, t):
        sums = []
        for g in range(CHUNK // 8):
            v = jnp.tanh(src[8 * g : 8 * g + 8, :] - t) + 1.0
            lvl = 0
            while sums and sums[-1][0] == lvl and lvl < 3:
                v = sums.pop()[1] + v
                lvl += 1
            if lvl == 3:
                acc = acc + v
            else:
                sums.append((lvl, v))
        return acc

    def total(p):
        cols = pl.ds(pl.multiple_of(p * PART, PART), PART)
        tsum = tsum_ref[:, cols]
        t = jnp.broadcast_to(tsum, (8, PART))

        def step(i, acc):
            k = p * steps + 2 * i
            score(k + 1, sb)
            acc = count(sa, acc, t)
            pick_history(p * (PART // 128) + i, 0)
            score(lax.rem(k + 2, parts * steps), sa)
            return count(sb, acc, t)

        acc = lax.fori_loop(0, steps // 2, step, jnp.zeros((8, PART), jnp.float32))
        mine = jnp.tanh(hsc[:, cols] - tsum) + 1.0
        return 0.5 * (jnp.sum(acc, axis=0, keepdims=True) - mine)

    def add(slots):
        out = slots[0]
        for i in range(1, n):
            out = out + slots[i]
        return out

    acopies = [
        exchange("items", peers, apart0, aslots0.at[me], as_.at[0], ar.at[0]),
        exchange("items", peers, apart1, aslots1.at[me], as_.at[1], ar.at[1]),
    ]

    def each(p, carry):
        @pl.when(p == 1)
        def _():
            wait(tcopies[1])
            tsum_ref[:, PART:] = add(tslots1)

        got = total(p)

        @pl.when(p < parts - 1)
        def _():
            apart0[:, pl.ds(pl.multiple_of(p * PART, PART), PART)] = got

        @pl.when(p == parts - 2)
        def _():
            aslots0[me] = apart0[...]
            start(acopies[0])

        @pl.when(p == parts - 1)
        def _():
            apart1[...] = got
            aslots1[me] = got
            start(acopies[1])

        return carry

    wait(tcopies[0])
    tsum_ref[:, :PART] = add(tslots0)
    lax.fori_loop(0, parts, each, 0)

    seen = jnp.max(jnp.where(hist_ref[...] == tgt_ref[...], 1.0, 0.0), axis=0, keepdims=True)
    hs = jnp.zeros((1, 128), jnp.float32)
    gs = jnp.zeros((1, 128), jnp.float32)
    for g, lo, hi, aslots in ((0, 0, u_dev - PART, aslots0), (1, u_dev - PART, u_dev, aslots1)):
        wait(acopies[g])
        rank = 1.0 + (add(aslots) - jnp.where(seen[:, lo:hi] > 0.5, 0.0, 0.5))
        out_ref[:, lo:hi] = jnp.log(rank)
        hit = jax.nn.sigmoid(10.5 - rank)
        gain = hit / jnp.log2(1.0 + rank)
        for b in range((hi - lo) // 128):
            hs = hs + hit[:, b * 128 : (b + 1) * 128]
            gs = gs + gain[:, b * 128 : (b + 1) * 128]
    mpart[:, :128] = hs
    mpart[:, 128:] = gs
    mslots[grp] = mpart[...]
    copies = exchange("users", mates, mpart, mslots.at[grp], ms, mr)
    start(copies)
    wait(copies)
    tot = mslots[0]
    for i in range(1, m):
        tot = tot + mslots[i]
    scale = 1.0 / (u_dev * m)
    hs = jnp.sum(tot[:, :128], axis=1, keepdims=True) * scale
    gs = jnp.sum(tot[:, 128:], axis=1, keepdims=True) * scale
    out_ref[:, u_dev:] = jnp.where(lax.broadcasted_iota(jnp.int32, (1, 128), 1) == 0, hs, gs)


def split(both, log_ref, met_ref):
    u_dev = log_ref.shape[0]
    log_ref[...] = both[0, :u_dev]
    met_ref[...] = both[0, u_dev : u_dev + 2]


def solution(mesh):
    n, m = mesh.shape["items"], mesh.shape["users"]

    def body(user_emb, item_emb, target, history):
        u_dev, dsh = user_emb.shape
        item_dev, d = item_emb.shape
        vmem = pl.BlockSpec(memory_space=pltpu.VMEM)
        hbm = pl.BlockSpec(memory_space=pltpu.HBM)
        dma = pltpu.SemaphoreType.DMA
        rest = u_dev - PART
        f32, bf16, i32 = jnp.float32, jnp.bfloat16, jnp.int32
        both = pl.pallas_call(
            functools.partial(kernel, n, m),
            out_shape=jax.ShapeDtypeStruct((1, u_dev + 128), f32),
            in_specs=[hbm, hbm, hbm, hbm],
            out_specs=vmem,
            scratch_shapes=[
                pltpu.VMEM((1, u_dev), i32),
                pltpu.VMEM((history.shape[1], u_dev), i32),
                pltpu.SMEM((1, u_dev), i32),
                pltpu.SMEM((1, u_dev), i32),
                pltpu.VMEM((2, n // 2, dsh, PART), bf16),
                pltpu.VMEM((2, n // 2, dsh, rest), bf16),
                pltpu.VMEM((d, u_dev), bf16),
                pltpu.VMEM((item_dev // TILE, TILE, d), bf16),
                pltpu.VMEM((u_dev, TILE, d), bf16),
                pltpu.VMEM((u_dev, TILE, d), bf16),
                pltpu.VMEM((CHUNK, PART), f32),
                pltpu.VMEM((CHUNK, PART), f32),
                pltpu.VMEM((1, u_dev), f32),
                pltpu.VMEM((1, PART), f32),
                pltpu.VMEM((1, rest), f32),
                pltpu.VMEM((n, 1, PART), f32),
                pltpu.VMEM((n, 1, rest), f32),
                pltpu.VMEM((1, u_dev), f32),
                pltpu.VMEM((1, u_dev), f32),
                pltpu.VMEM((1, rest), f32),
                pltpu.VMEM((1, PART), f32),
                pltpu.VMEM((n, 1, rest), f32),
                pltpu.VMEM((n, 1, PART), f32),
                pltpu.VMEM((1, 256), f32),
                pltpu.VMEM((m, 1, 256), f32),
                dma((PIECES,)),
                dma((6,)),
                dma((2, n - 1)), dma((2, n - 1)),
                dma((2, 1)), dma((2, 1)),
                dma((2, n - 1)), dma((2, n - 1)),
                dma((2, n - 1)), dma((2, n - 1)),
                dma((m - 1,)), dma((m - 1,)),
            ],
            compiler_params=pltpu.CompilerParams(
                collective_id=0, has_side_effects=True, vmem_limit_bytes=60 << 20
            ),
        )(user_emb.T, item_emb.reshape(item_dev // TILE, TILE, d), target.reshape(1, u_dev), history.T)
        return pl.pallas_call(
            split,
            out_shape=(jax.ShapeDtypeStruct((u_dev,), f32), jax.ShapeDtypeStruct((2,), f32)),
            in_specs=[vmem],
            out_specs=(vmem, vmem),
        )(both)

    return jax.shard_map(
        body,
        mesh=mesh,
        in_specs=(P("users", "items"), P("items", None), P("users"), P("users", None)),
        out_specs=(P("users"), P()),
        check_vma=False,
    )
```
